8 devices in a mesh: right: 4 (over z, y, x), left: 2 (over core).
Axes of the slice: x: 2, y: 2, z: 1, core: 2. Of those that a mesh axis runs over, the one named last changes fastest.
Arguments:
- psi_init: float32 [768, 2, 2, 768], P('left', None, None, 'right')
- env_left: float32 [768, 20, 768], P('left')
- env_right: float32 [768, 20, 768], P('right')
- mpo_pair: float32 [20, 20, 2, 2, 2, 2], replicated
Outputs:
- output 1: float32 [5], replicated
- output 2: float32 [5], replicated
- output 3: float32 [768, 2, 2, 768], P('left', None, None, 'right')
All inputs are finite; a program needn't handle non-finite values.
Results may differ from the reference program's by a relative error of at most 0.001.
Values sent between devices are 32-bit elements.
A program may use at most 1 GiB of HBM per device.

```python
import math
import jax
import jax.numpy as jnp
from jax import lax

PHYS_DIM = 2
MPO_DIM = 20
BOND_DIM = 768
KRYLOV_STEPS = 5
PREC_MODE = lax.Precision.HIGHEST


def sym_env(env_key, bond_dim, mpo_dim):
    key_mat, key_shift = jax.random.split(env_key)
    gauss_mat = jax.random.normal(key_mat, (bond_dim, mpo_dim, bond_dim), jnp.float32)
    sym_part = (gauss_mat + jnp.transpose(gauss_mat, (2, 1, 0))) / math.sqrt(2.0 * bond_dim)
    diag_shift = jax.random.normal(key_shift, (mpo_dim,), jnp.float32)
    eye_mat = jnp.eye(bond_dim, dtype=jnp.float32)
    return sym_part + eye_mat[:, None, :] * diag_shift[None, :, None]


def sym_mpo(mpo_key, mpo_dim, phys_dim):
    key_mat, key_diag = jax.random.split(mpo_key)
    gauss_mat = jax.random.normal(key_mat, (mpo_dim, mpo_dim, phys_dim, phys_dim, phys_dim, phys_dim), jnp.float32)
    sym_part = (gauss_mat + jnp.transpose(gauss_mat, (0, 1, 4, 5, 2, 3))) / (math.sqrt(2.0) * mpo_dim * phys_dim)
    diag_coef = jax.random.normal(key_diag, (mpo_dim, mpo_dim), jnp.float32) / mpo_dim
    eye_phys = jnp.eye(phys_dim * phys_dim, dtype=jnp.float32).reshape(phys_dim, phys_dim, phys_dim, phys_dim)
    return sym_part + diag_coef[:, :, None, None, None, None] * eye_phys[None, None]


def setup_inputs(seed: int = 0) -> dict:
    base_key = jax.random.key(seed)
    key_psi, key_left, key_right, key_mpo = jax.random.split(base_key, 4)
    psi_init = jax.random.normal(key_psi, (BOND_DIM, PHYS_DIM, PHYS_DIM, BOND_DIM), jnp.float32)
    return {
        "psi_init": psi_init,
        "env_left": sym_env(key_left, BOND_DIM, MPO_DIM),
        "env_right": sym_env(key_right, BOND_DIM, MPO_DIM),
        "mpo_pair": sym_mpo(key_mpo, MPO_DIM, PHYS_DIM),
    }


def apply_ham(in_vec, env_left, env_right, mpo_pair):
    stage_one = jnp.einsum("alc,asub->lcsub", env_left, in_vec, precision=PREC_MODE)
    stage_two = jnp.einsum("lrsutv,lcsub->rtvcb", mpo_pair, stage_one, precision=PREC_MODE)
    return jnp.einsum("rtvcb,bre->ctve", stage_two, env_right, precision=PREC_MODE)


def project_out(krylov_basis, residual, coeffs):
    for vec_idx, basis_vec in enumerate(krylov_basis):
        residual = residual - coeffs[vec_idx] * basis_vec
    return residual


def reference(psi_init, env_left, env_right, mpo_pair):
    init_norm = jnp.sqrt(jnp.sum(psi_init * psi_init))
    krylov_basis = [psi_init / init_norm]
    alpha_list = []
    beta_list = []
    for step_idx in range(KRYLOV_STEPS):
        residual = apply_ham(krylov_basis[-1], env_left, env_right, mpo_pair)
        first_pass = jnp.stack([jnp.sum(basis_vec * residual) for basis_vec in krylov_basis])
        alpha_list.append(first_pass[-1])
        residual = project_out(krylov_basis, residual, first_pass)
        second_pass = jnp.stack([jnp.sum(basis_vec * residual) for basis_vec in krylov_basis])
        residual = project_out(krylov_basis, residual, second_pass)
        beta_val = jnp.sqrt(jnp.sum(residual * residual))
        beta_list.append(beta_val)
        krylov_basis.append(residual / beta_val)
    out_scale = math.sqrt(float(psi_init.size))
    return jnp.stack(alpha_list), jnp.stack(beta_list), krylov_basis[-1] * out_scale
```

```python
import math
import jax
import jax.numpy as jnp
from jax import lax
from jax.experimental import pallas as pl
from jax.experimental.pallas import tpu as pltpu
from jax.sharding import PartitionSpec as P

F32, BF16 = jnp.float32, jnp.bfloat16
MESH = pl.DeviceIdType.MESH
KRYLOV_STEPS = 5
N_RIGHT, N_LEFT = 4, 2
N_DEV = N_RIGHT * N_LEFT
BOND = 768
MPO = 20
ROWS = BOND // N_LEFT
COLS = BOND // N_RIGHT
LB = 64
NBLK = ROWS // LB
HALF = LB // 2
CS, CX = LB + 8, HALF + 8
UNITS = 16
K_FIRST, K_SECOND, K_NORM = 0, 1, 2


def split3(x):
    hi = x.astype(BF16)
    rest = x - hi.astype(F32)
    mid = rest.astype(BF16)
    low = (rest - mid.astype(F32)).astype(BF16)
    return hi, mid, low


def dot(a, b):
    return jnp.dot(a, b, preferred_element_type=F32)


def dot6(a, b):
    return (dot(a[0], b[0]) + (dot(a[0], b[1]) + dot(a[1], b[0]))
            + (dot(a[0], b[2]) + dot(a[1], b[1]) + dot(a[2], b[0])))


def lane_pair(x0, x1):
    left = lax.broadcasted_iota(jnp.int32, x0.shape, 1) < 64
    return (jnp.where(left, x0, pltpu.roll(x1, 64, 1)),
            jnp.where(left, pltpu.roll(x0, 64, 1), x1))


def kernel(psi, l_hi, l_mid, l_low, r_hi, r_mid, r_low, w_main, w_extra,
           out_small, out_psi,
           lb, rm, rx, vs, t1m, t1x, zm, zx, zs, yb, sb, rv, basis, u, ab, coef, scal,
           l_sem, r_sem, io_sem, rs_send, rs_recv, pu_send, pu_recv, ar_send, ar_recv):
    my_r, my_l = lax.axis_index("right"), lax.axis_index("left")
    me = my_r * N_LEFT + my_l
    own0 = pl.multiple_of(my_l * ROWS, ROWS)
    oth0 = pl.multiple_of((1 - my_l) * ROWS, ROWS)
    partner = (my_r, 1 - my_l)
    odd = lax.rem(my_r, 2)
    main0 = pl.multiple_of(odd * 64, 64)
    extra0 = pl.multiple_of((1 - odd) * 128, 64)
    l_hbm = (l_hi, l_mid, l_low)
    r_hbm = (r_hi, r_mid, r_low)

    def l_copies(blk):
        row = pl.multiple_of(blk * LB, LB)
        return [pltpu.make_async_copy(l_hbm[i].at[:, pl.ds(row, LB), :], lb.at[i], l_sem.at[i])
                for i in range(3)]

    def r_copies():
        return ([pltpu.make_async_copy(r_hbm[i].at[:, pl.ds(main0, 128), :], rm.at[i], r_sem.at[i])
                 for i in range(3)]
                + [pltpu.make_async_copy(r_hbm[i].at[:, pl.ds(extra0, 64), :], rx.at[i], r_sem.at[3 + i])
                   for i in range(3)])

    def piece_copies(blk):
        slot = lax.rem(blk, 2)
        row = pl.multiple_of(blk * LB, LB)
        out = []
        for p in range(1, N_RIGHT):
            to = lax.rem(my_r + p, N_RIGHT)
            out.append(pltpu.make_async_remote_copy(
                src_ref=sb.at[slot, to], dst_ref=rv.at[p - 1, pl.ds(row, LB), :],
                send_sem=rs_send.at[p - 1, slot], recv_sem=rs_recv.at[p - 1, blk],
                device_id=(to, my_l), device_id_type=MESH))
        return out

    def partner_copy(blk):
        row = pl.multiple_of(own0 + blk * LB, LB)
        return pltpu.make_async_remote_copy(
            src_ref=u.at[pl.ds(row, LB), :], dst_ref=u.at[pl.ds(row, LB), :],
            send_sem=pu_send.at[blk], recv_sem=pu_recv.at[blk],
            device_id=partner, device_id_type=MESH)

    def sum_copies(kind):
        out = []
        for p in range(1, N_DEV):
            to = lax.rem(me + p, N_DEV)
            out.append(pltpu.make_async_remote_copy(
                src_ref=ab.at[kind, me], dst_ref=ab.at[kind, me],
                send_sem=ar_send.at[kind, p - 1], recv_sem=ar_recv.at[kind, p - 1],
                device_id=(to // N_LEFT, lax.rem(to, N_LEFT)), device_id_type=MESH))
        return out

    def sum_start(kind):
        for copy in sum_copies(kind):
            copy.start()

    def sum_finish(kind):
        for copy in sum_copies(kind):
            copy.wait()
        total = ab[kind, 0]
        for d in range(1, N_DEV):
            total = total + ab[kind, d]
        return jnp.broadcast_to(jnp.sum(total, axis=1, keepdims=True), (8, BOND))

    def put_row(kind, i, acc):
        rows = jnp.sum(acc, axis=0, keepdims=True)
        part = rows[:, 0:128]
        for n in range(1, acc.shape[1] // 128):
            part = part + rows[:, n * 128:(n + 1) * 128]
        ab[kind, me, pl.ds(i, 1), :] = part

    for copy in l_copies(0):
        copy.start()
    for copy in r_copies():
        copy.start()
    psi_in = pltpu.make_async_copy(psi, u.at[pl.ds(own0, ROWS), :], io_sem)
    psi_in.start()
    for kind in range(3):
        ab[kind, me] = jnp.zeros((8, 128), F32)
    coef[...] = jnp.zeros_like(coef)
    scal[...] = jnp.zeros_like(scal)
    out_small[...] = jnp.zeros_like(out_small)

    def clear(i, _):
        row = pl.multiple_of(i * 8, 8)
        for n in range(1, KRYLOV_STEPS):
            basis[n, pl.ds(row, 8), :] = jnp.zeros((8, BOND), F32)
        return 0
    lax.fori_loop(0, BOND // 8, clear, 0)

    barrier = pltpu.get_barrier_semaphore()
    for p in range(1, N_DEV):
        to = lax.rem(me + p, N_DEV)
        pl.semaphore_signal(barrier, inc=1, device_id=(to // N_LEFT, lax.rem(to, N_LEFT)),
                            device_id_type=MESH)
    pl.semaphore_wait(barrier, N_DEV - 1)

    def finalize(dst):
        def rows(base, with_norm):
            def body(i, acc):
                row = pl.multiple_of(base + i * 16, 16)
                out = []
                for n in range(2):
                    cols = pl.ds(n * 384, 384)
                    x = u[pl.ds(row, 16), cols]
                    for m in range(KRYLOV_STEPS):
                        x = x - coef[1, pl.ds(m, 1), cols] * basis[m, pl.ds(row, 16), cols]
                    x = x * scal[pl.ds(0, 1), cols]
                    basis[dst, pl.ds(row, 16), cols] = x
                    for t, part in enumerate(split3(x)):
                        vs[t, pl.ds(row, 16), cols] = part
                    if with_norm:
                        x2 = x * x
                        out.append(acc[n] + (x2[:8] + x2[8:]))
                return tuple(out) if with_norm else 0
            init = (jnp.zeros((8, 384), F32),) * 2 if with_norm else 0
            return lax.fori_loop(0, ROWS // 16, body, init)
        acc = rows(own0, True)
        put_row(K_NORM, 0, acc[0] + acc[1])
        rows(oth0, False)
        sum_start(K_NORM)

    def norm_scale():
        root = jnp.sqrt(scal[pl.ds(2, 1), :])
        scal[pl.ds(1, 1), :] = root
        scal[pl.ds(0, 1), :] = 1.0 / root

    psi_in.wait()

    def greet(blk, _):
        partner_copy(blk).start()
        return 0
    lax.fori_loop(0, NBLK, greet, 0)

    def square(i, acc):
        x = u[pl.ds(pl.multiple_of(own0 + i * 8, 8), 8), :]
        return acc + x * x
    put_row(K_SECOND, 5, lax.fori_loop(0, ROWS // 8, square, jnp.zeros((8, BOND), F32)))
    sum_start(K_SECOND)

    def partner_wait(blk, _):
        partner_copy(blk).wait()
        return 0
    lax.fori_loop(0, NBLK, partner_wait, 0)
    scal[pl.ds(2, 1), :] = sum_finish(K_SECOND)[5:6, :]
    norm_scale()
    finalize(0)

    def stage_one(i, _):
        l0 = i * 4
        a = [lb[t, pl.ds(l0, 4)].reshape(4 * LB, BOND) for t in range(3)]
        for n in range(3):
            t1 = dot6(a, [vs[t, :, n * 256:(n + 1) * 256] for t in range(3)])
            for h in range(2):
                t1h = t1[:, h * 128:(h + 1) * 128]
                for d in range(4):
                    x = t1h[d * LB:(d + 1) * LB]
                    if n < 2:
                        row = pl.multiple_of(((2 * n + h) * MPO + l0 + d) * CS, 8)
                        t1m[pl.ds(row, LB), :] = x
                    else:
                        row = pl.multiple_of((h * MPO + l0 + d) * 2 * CX, 8)
                        x0, x1 = lane_pair(x[:HALF], x[HALF:])
                        t1x[pl.ds(row, HALF), :] = x0
                        t1x[pl.ds(row + CX, HALF), :] = x1
        return 0

    def mpo_units(src, dst, w_ref, stride):
        def body(i, _):
            for n in range(UNITS):
                c = (i * UNITS + n) * 2
                x = jnp.concatenate([src[pl.ds(c, 80, stride=stride), :],
                                     src[pl.ds(c + 1, 80, stride=stride), :]], axis=1)
                t2 = dot(w_ref[...], jnp.concatenate(split3(x), axis=0))
                t2 = t2[0:80] + (t2[80:160] + t2[160:240])
                dst[pl.ds(c, 80, stride=stride), :] = t2[:, :128]
                dst[pl.ds(c + 1, 80, stride=stride), :] = t2[:, 128:]
            return 0
        return body

    def gather_main(r, _):
        cols = pl.ds(pl.multiple_of(r * 128, 128), 128)
        for t in range(4):
            x = zm[pl.ds(pl.multiple_of((r * 4 + t) * CS, 8), LB), :]
            for i, part in enumerate(split3(x)):
                zs[i, t * LB:(t + 1) * LB, cols] = part
        return 0

    def gather_extra(q, _):
        cols = pl.ds(pl.multiple_of(MPO * 128 + q * 128, 128), 128)
        for t in range(4):
            x0 = zx[pl.ds(pl.multiple_of((q * 8 + t) * CX, 8), HALF), :]
            x1 = zx[pl.ds(pl.multiple_of((q * 8 + 4 + t) * CX, 8), HALF), :]
            x = jnp.concatenate(lane_pair(x0, x1), axis=0)
            for i, part in enumerate(split3(x)):
                zs[i, t * LB:(t + 1) * LB, cols] = part
        return 0

    def stage_three(n, _):
        cols = pl.ds(pl.multiple_of(n * 256, 256), 256)
        b = [jnp.concatenate([rm[t, :, :, cols].reshape(MPO * 128, 256),
                              rx[t, :, :, cols].reshape(MPO * 64, 256)], axis=0) for t in range(3)]
        yb[:, cols] = dot6([zs[t] for t in range(3)], b)
        return 0

    def pack(blk):
        slot = lax.rem(blk, 2)
        for to in range(N_RIGHT):
            lane = (0, 2, 3, 5)[to] * 128
            for t in range(4):
                sb[slot, to, :, t * 128:(t + 1) * 128] = yb[t * LB:(t + 1) * LB, lane:lane + 128]
        for pair in range(2):
            lane = (1, 4)[pair] * 128
            for h in range(2):
                y0 = yb[(2 * h) * LB:(2 * h + 1) * LB, lane:lane + 128]
                y1 = yb[(2 * h + 1) * LB:(2 * h + 2) * LB, lane:lane + 128]
                for k, x in enumerate(lane_pair(y0, y1)):
                    sb[slot, 2 * pair + k, :, 512 + h * 128:640 + h * 128] = x

    def reduce(blk):
        slot = lax.rem(blk, 2)
        for copy in piece_copies(blk):
            copy.wait()
        row = pl.multiple_of(blk * LB, LB)
        x = (sb[slot, my_r] + rv[0, pl.ds(row, LB), :]) + (rv[1, pl.ds(row, LB), :] + rv[2, pl.ds(row, LB), :])
        u[pl.ds(pl.multiple_of(own0 + row, LB), LB), :] = x * scal[pl.ds(3, 1), :]
        partner_copy(blk).start()

    def finish_norm(step):
        total = sum_finish(K_NORM)[0:1, :]
        root = jnp.sqrt(total)
        scal[pl.ds(3, 1), :] = 1.0 / root
        out_small[pl.ds(8 + step, 1), :] = (scal[pl.ds(1, 1), :] * root)[:, :128]

    def krylov_step(step, _):
        def block(blk, _):
            for copy in l_copies(blk):
                copy.wait()
            lax.fori_loop(0, MPO // 4, stage_one, 0)
            for copy in l_copies(lax.rem(blk + 1, NBLK)):
                copy.start()
            lax.fori_loop(0, LB // 2 // UNITS, mpo_units(t1m, zm, w_main, CS), 0)
            lax.fori_loop(0, HALF // 2 // UNITS, mpo_units(t1x, zx, w_extra, CX), 0)
            lax.fori_loop(0, MPO, gather_main, 0)
            lax.fori_loop(0, MPO // 2, gather_extra, 0)

            @pl.when((step == 0) & (blk == 0))
            def _():
                for copy in r_copies():
                    copy.wait()

            lax.fori_loop(0, 3, stage_three, 0)
            pack(blk)
            for copy in piece_copies(blk):
                copy.start()

            @pl.when(blk == 0)
            def _():
                finish_norm(step)

                def rescale(i, _):
                    row = pl.multiple_of(i * 16, 16)
                    basis[step, pl.ds(row, 16), :] = basis[step, pl.ds(row, 16), :] * scal[pl.ds(3, 1), :]
                    return 0
                lax.fori_loop(0, BOND // 16, rescale, 0)

            @pl.when(blk > 0)
            def _():
                reduce(blk - 1)
            return 0

        lax.fori_loop(0, NBLK, block, 0)
        reduce(jnp.int32(NBLK - 1))

        def first(i, acc):
            row = pl.multiple_of(own0 + i * 8, 8)
            x = u[pl.ds(row, 8), :]
            return tuple(acc[m] + x * basis[m, pl.ds(row, 8), :] for m in range(KRYLOV_STEPS))
        acc = lax.fori_loop(0, ROWS // 8, first, (jnp.zeros((8, BOND), F32),) * KRYLOV_STEPS)
        for m in range(KRYLOV_STEPS):
            put_row(K_FIRST, m, acc[m])
        sum_start(K_FIRST)
        coef[0] = sum_finish(K_FIRST)
        mine = lax.broadcasted_iota(jnp.int32, (8, 128), 0) == step
        out_small[pl.ds(step, 1), :] = jnp.sum(jnp.where(mine, coef[0, :, 0:128], 0.0), axis=0, keepdims=True)

        def project(base, with_dots):
            def body(i, acc):
                row = pl.multiple_of(base + i * 8, 8)
                new = []
                for n in range(2):
                    cols = pl.ds(n * 384, 384)
                    x = u[pl.ds(row, 8), cols]
                    vecs = [basis[m, pl.ds(row, 8), cols] for m in range(KRYLOV_STEPS)]
                    for m in range(KRYLOV_STEPS):
                        x = x - coef[0, pl.ds(m, 1), cols] * vecs[m]
                    u[pl.ds(row, 8), cols] = x
                    if with_dots:
                        prods = [x * vec for vec in vecs] + [x * x]
                        new.append(prods)
                if not with_dots:
                    return 0
                return tuple(a + (p0 + p1) for a, p0, p1 in zip(acc, new[0], new[1]))
            init = (jnp.zeros((8, 384), F32),) * (KRYLOV_STEPS + 1) if with_dots else 0
            return lax.fori_loop(0, ROWS // 8, body, init)
        lax.fori_loop(0, NBLK, partner_wait, 0)
        acc = project(own0, True)
        for m in range(KRYLOV_STEPS + 1):
            put_row(K_SECOND, m, acc[m])
        sum_start(K_SECOND)
        project(oth0, False)
        total = sum_finish(K_SECOND)
        coef[1, 0:5] = total[0:5]
        scal[pl.ds(2, 1), :] = total[5:6, :]
        norm_scale()
        finalize(lax.rem(step + 1, KRYLOV_STEPS))
        return 0

    lax.fori_loop(0, KRYLOV_STEPS, krylov_step, 0)

    finish_norm(KRYLOV_STEPS)
    for copy in l_copies(0):
        copy.wait()

    def scale_out(i, _):
        row = pl.multiple_of(own0 + i * 16, 16)
        u[pl.ds(row, 16), :] = basis[0, pl.ds(row, 16), :] * scal[pl.ds(3, 1), :] * math.sqrt(4.0 * BOND * BOND)
        return 0
    lax.fori_loop(0, ROWS // 16, scale_out, 0)
    psi_out = pltpu.make_async_copy(u.at[pl.ds(own0, ROWS), :], out_psi, io_sem)
    psi_out.start()
    psi_out.wait()


def split3_xla(x):
    hi = lax.reduce_precision(x, 8, 7)
    rest = x - hi
    mid = lax.reduce_precision(rest, 8, 7)
    low = rest - mid
    return hi.astype(BF16), mid.astype(BF16), low.astype(BF16)


def mpo_matrix(w_mat):
    w0, w1, w2 = split3_xla(w_mat)
    zero = jnp.zeros_like(w0)
    return jnp.concatenate([jnp.concatenate([w0, w0, w0], axis=1),
                            jnp.concatenate([w1, w1, zero], axis=1),
                            jnp.concatenate([w2, zero, zero], axis=1)], axis=0)


def solution(mesh):
    psi_spec = P("left", None, None, "right")

    def local_fn(psi, env_left, env_right, mpo):
        odd = lax.rem(lax.axis_index("right"), 2) == 1
        psi4 = psi.reshape(ROWS, 4, COLS)
        main = jnp.where(odd, psi4[:, :, 64:], psi4[:, :, :128]).reshape(ROWS, 512)
        extra = jnp.where(odd, psi4[:, :, :64], psi4[:, :, 128:]).reshape(ROWS, 256)
        psi_q = jnp.concatenate([main, extra], axis=1)
        lefts = split3_xla(jnp.transpose(env_left, (1, 0, 2)))
        rights = split3_xla(jnp.transpose(env_right, (1, 0, 2)))
        w_rows = jnp.transpose(mpo.reshape(MPO, MPO, 4, 4), (1, 3, 2, 0)).reshape(80, 80)
        w_pairs = jnp.transpose(mpo.reshape(MPO, MPO, 2, 2, 4), (1, 4, 2, 0, 3)).reshape(80, 80)

        vmem = pl.BlockSpec(memory_space=pltpu.VMEM)
        hbm = pl.BlockSpec(memory_space=pl.ANY)
        dma = pltpu.SemaphoreType.DMA
        small, psi_new = pl.pallas_call(
            kernel,
            out_shape=(jax.ShapeDtypeStruct((16, 128), F32), jax.ShapeDtypeStruct((ROWS, BOND), F32)),
            in_specs=[hbm] * 7 + [vmem] * 2,
            out_specs=(vmem, hbm),
            scratch_shapes=[
                pltpu.VMEM((3, MPO, LB, BOND), BF16),
                pltpu.VMEM((3, MPO, 128, BOND), BF16),
                pltpu.VMEM((3, MPO, 64, BOND), BF16),
                pltpu.VMEM((3, BOND, BOND), BF16),
                pltpu.VMEM((80 * CS, 128), F32),
                pltpu.VMEM((80 * CX, 128), F32),
                pltpu.VMEM((80 * CS, 128), F32),
                pltpu.VMEM((80 * CX, 128), F32),
                pltpu.VMEM((3, 4 * LB, MPO * COLS), BF16),
                pltpu.VMEM((4 * LB, BOND), F32),
                pltpu.VMEM((2, N_RIGHT, LB, BOND), F32),
                pltpu.VMEM((N_RIGHT - 1, ROWS, BOND), F32),
                pltpu.VMEM((KRYLOV_STEPS, BOND, BOND), F32),
                pltpu.VMEM((BOND, BOND), F32),
                pltpu.VMEM((3, N_DEV, 8, 128), F32),
                pltpu.VMEM((2, 8, BOND), F32),
                pltpu.VMEM((8, BOND), F32),
                dma((3,)), dma((6,)), dma,
                dma((N_RIGHT - 1, 2)), dma((N_RIGHT - 1, NBLK)),
                dma((NBLK,)), dma((NBLK,)),
                dma((3, N_DEV - 1)), dma((3, N_DEV - 1)),
            ],
            compiler_params=pltpu.CompilerParams(
                collective_id=0, has_side_effects=True, vmem_limit_bytes=67_000_000),
            name="lanczos",
        )(psi_q, *lefts, *rights, mpo_matrix(w_rows), mpo_matrix(w_pairs))

        main = psi_new[:, :512].reshape(ROWS, 4, 128)
        extra = psi_new[:, 512:].reshape(ROWS, 4, 64)
        psi_next = jnp.where(odd, jnp.concatenate([extra, main], axis=2),
                             jnp.concatenate([main, extra], axis=2)).reshape(ROWS, 2, 2, COLS)
        return small[0:5, 0], small[9:14, 0], psi_next

    return jax.shard_map(
        local_fn,
        mesh=mesh,
        in_specs=(psi_spec, P("left", None, None), P("right", None, None), P()),
        out_specs=(P(), P(), psi_spec),
        check_vma=False,
    )
```

```python
import math
import jax
import jax.numpy as jnp
from jax import lax
from jax.experimental import pallas as pl
from jax.experimental.pallas import tpu as pltpu
from jax.sharding import PartitionSpec as P

F32, BF16 = jnp.float32, jnp.bfloat16
MESH = pl.DeviceIdType.MESH
KRYLOV_STEPS = 5
N_RIGHT, N_LEFT = 4, 2
N_DEV = N_RIGHT * N_LEFT
BOND = 768
MPO = 20
ROWS = BOND // N_LEFT
COLS = BOND // N_RIGHT
LB = 64
NBLK = ROWS // LB
HALF = LB // 2
CS, CX = LB + 8, HALF + 8
LC = 20
UNITS = 16
K_FIRST, K_SECOND, K_NORM = 0, 1, 2


def split3(x):
    hi = x.astype(BF16)
    rest = x - hi.astype(F32)
    mid = rest.astype(BF16)
    low = (rest - mid.astype(F32)).astype(BF16)
    return hi, mid, low


def dot(a, b):
    return jnp.dot(a, b, preferred_element_type=F32)


def dot6(a, b):
    return (dot(a[0], b[0]) + (dot(a[0], b[1]) + dot(a[1], b[0]))
            + (dot(a[0], b[2]) + dot(a[1], b[1]) + dot(a[2], b[0])))


def lane_pair(x0, x1):
    left = lax.broadcasted_iota(jnp.int32, x0.shape, 1) < 64
    return (jnp.where(left, x0, pltpu.roll(x1, 64, 1)),
            jnp.where(left, pltpu.roll(x0, 64, 1), x1))


def kernel(psi, l_hi, l_mid, l_low, r_hi, r_mid, r_low, w_main, w_extra,
           out_small, out_psi,
           lb, rm, rx, vs, t1m, t1x, zm, zx, zs, yb, sb, rv, basis, u, ab, coef, scal,
           l_sem, r_sem, io_sem, rs_send, rs_recv, pu_send, pu_recv, ar_send, ar_recv):
    my_r, my_l = lax.axis_index("right"), lax.axis_index("left")
    me = my_r * N_LEFT + my_l
    own0 = pl.multiple_of(my_l * ROWS, ROWS)
    oth0 = pl.multiple_of((1 - my_l) * ROWS, ROWS)
    partner = (my_r, 1 - my_l)
    odd = lax.rem(my_r, 2)
    main0 = pl.multiple_of(odd * 64, 64)
    extra0 = pl.multiple_of((1 - odd) * 128, 64)
    l_hbm = (l_hi, l_mid, l_low)
    r_hbm = (r_hi, r_mid, r_low)

    def l_copies(blk):
        row = pl.multiple_of(blk * LB, LB)
        return [pltpu.make_async_copy(l_hbm[i].at[:, pl.ds(row, LB), :], lb.at[i], l_sem.at[i])
                for i in range(3)]

    def r_copies():
        return ([pltpu.make_async_copy(r_hbm[i].at[:, pl.ds(main0, 128), :], rm.at[i], r_sem.at[i])
                 for i in range(3)]
                + [pltpu.make_async_copy(r_hbm[i].at[:, pl.ds(extra0, 64), :], rx.at[i], r_sem.at[3 + i])
                   for i in range(3)])

    def piece_copies(blk):
        slot = lax.rem(blk, 2)
        row = pl.multiple_of(blk * LB, LB)
        out = []
        for p in range(1, N_RIGHT):
            to = lax.rem(my_r + p, N_RIGHT)
            out.append(pltpu.make_async_remote_copy(
                src_ref=sb.at[slot, to], dst_ref=rv.at[p - 1, pl.ds(row, LB), :],
                send_sem=rs_send.at[p - 1, slot], recv_sem=rs_recv.at[p - 1, blk],
                device_id=(to, my_l), device_id_type=MESH))
        return out

    def partner_copy(blk):
        row = pl.multiple_of(own0 + blk * LB, LB)
        return pltpu.make_async_remote_copy(
            src_ref=u.at[pl.ds(row, LB), :], dst_ref=u.at[pl.ds(row, LB), :],
            send_sem=pu_send.at[blk], recv_sem=pu_recv.at[blk],
            device_id=partner, device_id_type=MESH)

    def sum_copies(kind):
        out = []
        for p in range(1, N_DEV):
            to = lax.rem(me + p, N_DEV)
            out.append(pltpu.make_async_remote_copy(
                src_ref=ab.at[kind, me], dst_ref=ab.at[kind, me],
                send_sem=ar_send.at[kind, p - 1], recv_sem=ar_recv.at[kind, p - 1],
                device_id=(to // N_LEFT, lax.rem(to, N_LEFT)), device_id_type=MESH))
        return out

    def sum_start(kind):
        for copy in sum_copies(kind):
            copy.start()

    def sum_finish(kind):
        for copy in sum_copies(kind):
            copy.wait()
        total = ab[kind, 0]
        for d in range(1, N_DEV):
            total = total + ab[kind, d]
        return jnp.broadcast_to(jnp.sum(total, axis=1, keepdims=True), (8, BOND))

    def put_row(kind, i, acc):
        rows = jnp.sum(acc, axis=0, keepdims=True)
        part = rows[:, 0:128]
        for n in range(1, acc.shape[1] // 128):
            part = part + rows[:, n * 128:(n + 1) * 128]
        ab[kind, me, pl.ds(i, 1), :] = part

    for copy in l_copies(0):
        copy.start()
    for copy in r_copies():
        copy.start()
    psi_in = pltpu.make_async_copy(psi, u.at[pl.ds(own0, ROWS), :], io_sem)
    psi_in.start()
    for kind in range(3):
        ab[kind, me] = jnp.zeros((8, 128), F32)
    coef[...] = jnp.zeros_like(coef)
    scal[...] = jnp.zeros_like(scal)
    out_small[...] = jnp.zeros_like(out_small)

    def clear(i, _):
        row = pl.multiple_of(i * 8, 8)
        for n in range(1, KRYLOV_STEPS):
            basis[n, pl.ds(row, 8), :] = jnp.zeros((8, BOND), F32)
        return 0
    lax.fori_loop(0, BOND // 8, clear, 0)

    barrier = pltpu.get_barrier_semaphore()
    for p in range(1, N_DEV):
        to = lax.rem(me + p, N_DEV)
        pl.semaphore_signal(barrier, inc=1, device_id=(to // N_LEFT, lax.rem(to, N_LEFT)),
                            device_id_type=MESH)
    pl.semaphore_wait(barrier, N_DEV - 1)

    def finalize(dst):
        def rows(base, with_norm):
            def body(i, acc):
                row = pl.multiple_of(base + i * 16, 16)
                out = []
                for n in range(2):
                    cols = pl.ds(n * 384, 384)
                    x = u[pl.ds(row, 16), cols]
                    for m in range(KRYLOV_STEPS):
                        x = x - coef[1, pl.ds(m, 1), cols] * basis[m, pl.ds(row, 16), cols]
                    x = x * scal[pl.ds(0, 1), cols]
                    basis[dst, pl.ds(row, 16), cols] = x
                    for t, part in enumerate(split3(x)):
                        vs[t, pl.ds(row, 16), cols] = part
                    if with_norm:
                        x2 = x * x
                        out.append(acc[n] + (x2[:8] + x2[8:]))
                return tuple(out) if with_norm else 0
            init = (jnp.zeros((8, 384), F32),) * 2 if with_norm else 0
            return lax.fori_loop(0, ROWS // 16, body, init, unroll=4)
        acc = rows(own0, True)
        put_row(K_NORM, 0, acc[0] + acc[1])
        rows(oth0, False)
        sum_start(K_NORM)

    def norm_scale():
        root = jnp.sqrt(scal[pl.ds(2, 1), :])
        scal[pl.ds(1, 1), :] = root
        scal[pl.ds(0, 1), :] = 1.0 / root

    psi_in.wait()

    def greet(blk, _):
        partner_copy(blk).start()
        return 0
    lax.fori_loop(0, NBLK, greet, 0)

    def square(i, acc):
        x = u[pl.ds(pl.multiple_of(own0 + i * 8, 8), 8), :]
        return acc + x * x
    put_row(K_SECOND, 5, lax.fori_loop(0, ROWS // 8, square, jnp.zeros((8, BOND), F32)))
    sum_start(K_SECOND)

    def partner_wait(blk, _):
        partner_copy(blk).wait()
        return 0
    lax.fori_loop(0, NBLK, partner_wait, 0)
    scal[pl.ds(2, 1), :] = sum_finish(K_SECOND)[5:6, :]
    norm_scale()
    finalize(0)

    def stage_one(i, _):
        l0 = i * LC
        a = [lb[t, pl.ds(l0, LC)].reshape(LC * LB, BOND) for t in range(3)]
        for n in range(3):
            t1 = dot6(a, [vs[t, :, n * 256:(n + 1) * 256] for t in range(3)])
            for h in range(2):
                t1h = t1[:, h * 128:(h + 1) * 128]
                for d in range(LC):
                    x = t1h[d * LB:(d + 1) * LB]
                    if n < 2:
                        row = pl.multiple_of(((2 * n + h) * MPO + l0 + d) * CS, 8)
                        t1m[pl.ds(row, LB), :] = x
                    else:
                        row = pl.multiple_of((h * MPO + l0 + d) * 2 * CX, 8)
                        x0, x1 = lane_pair(x[:HALF], x[HALF:])
                        t1x[pl.ds(row, HALF), :] = x0
                        t1x[pl.ds(row + CX, HALF), :] = x1
        return 0

    def mpo_units(src, dst, w_ref, stride):
        def body(i, _):
            for n in range(UNITS):
                c = (i * UNITS + n) * 2
                x = jnp.concatenate([src[pl.ds(c, 80, stride=stride), :],
                                     src[pl.ds(c + 1, 80, stride=stride), :]], axis=1)
                t2 = dot(w_ref[...], jnp.concatenate(split3(x), axis=0))
                t2 = t2[0:80] + (t2[80:160] + t2[160:240])
                dst[pl.ds(c, 80, stride=stride), :] = t2[:, :128]
                dst[pl.ds(c + 1, 80, stride=stride), :] = t2[:, 128:]
            return 0
        return body

    def gather_main(r, _):
        cols = pl.ds(pl.multiple_of(r * 128, 128), 128)
        for t in range(4):
            x = zm[pl.ds(pl.multiple_of((r * 4 + t) * CS, 8), LB), :]
            for i, part in enumerate(split3(x)):
                zs[i, t * LB:(t + 1) * LB, cols] = part
        return 0

    def gather_extra(q, _):
        cols = pl.ds(pl.multiple_of(MPO * 128 + q * 128, 128), 128)
        for t in range(4):
            x0 = zx[pl.ds(pl.multiple_of((q * 8 + t) * CX, 8), HALF), :]
            x1 = zx[pl.ds(pl.multiple_of((q * 8 + 4 + t) * CX, 8), HALF), :]
            x = jnp.concatenate(lane_pair(x0, x1), axis=0)
            for i, part in enumerate(split3(x)):
                zs[i, t * LB:(t + 1) * LB, cols] = part
        return 0

    def stage_three(n, _):
        cols = pl.ds(pl.multiple_of(n * 256, 256), 256)
        b = [jnp.concatenate([rm[t, :, :, cols].reshape(MPO * 128, 256),
                              rx[t, :, :, cols].reshape(MPO * 64, 256)], axis=0) for t in range(3)]
        yb[:, cols] = dot6([zs[t] for t in range(3)], b)
        return 0

    def pack(blk):
        slot = lax.rem(blk, 2)
        for to in range(N_RIGHT):
            lane = (0, 2, 3, 5)[to] * 128
            for t in range(4):
                sb[slot, to, :, t * 128:(t + 1) * 128] = yb[t * LB:(t + 1) * LB, lane:lane + 128]
        for pair in range(2):
            lane = (1, 4)[pair] * 128
            for h in range(2):
                y0 = yb[(2 * h) * LB:(2 * h + 1) * LB, lane:lane + 128]
                y1 = yb[(2 * h + 1) * LB:(2 * h + 2) * LB, lane:lane + 128]
                for k, x in enumerate(lane_pair(y0, y1)):
                    sb[slot, 2 * pair + k, :, 512 + h * 128:640 + h * 128] = x

    def reduce(blk):
        slot = lax.rem(blk, 2)
        for copy in piece_copies(blk):
            copy.wait()
        row = pl.multiple_of(blk * LB, LB)
        x = (sb[slot, my_r] + rv[0, pl.ds(row, LB), :]) + (rv[1, pl.ds(row, LB), :] + rv[2, pl.ds(row, LB), :])
        u[pl.ds(pl.multiple_of(own0 + row, LB), LB), :] = x * scal[pl.ds(3, 1), :]
        partner_copy(blk).start()

    def finish_norm(step):
        total = sum_finish(K_NORM)[0:1, :]
        root = jnp.sqrt(total)
        scal[pl.ds(3, 1), :] = 1.0 / root
        out_small[pl.ds(8 + step, 1), :] = (scal[pl.ds(1, 1), :] * root)[:, :128]

    def krylov_step(step, _):
        def block(blk, _):
            for copy in l_copies(blk):
                copy.wait()
            lax.fori_loop(0, MPO // LC, stage_one, 0)
            for copy in l_copies(lax.rem(blk + 1, NBLK)):
                copy.start()
            lax.fori_loop(0, LB // 2 // UNITS, mpo_units(t1m, zm, w_main, CS), 0)
            lax.fori_loop(0, HALF // 2 // UNITS, mpo_units(t1x, zx, w_extra, CX), 0)
            lax.fori_loop(0, MPO, gather_main, 0, unroll=MPO)
            lax.fori_loop(0, MPO // 2, gather_extra, 0, unroll=MPO // 2)

            @pl.when((step == 0) & (blk == 0))
            def _():
                for copy in r_copies():
                    copy.wait()

            lax.fori_loop(0, 3, stage_three, 0, unroll=3)
            pack(blk)
            for copy in piece_copies(blk):
                copy.start()

            @pl.when(blk == 0)
            def _():
                finish_norm(step)

                def rescale(i, _):
                    row = pl.multiple_of(i * 16, 16)
                    basis[step, pl.ds(row, 16), :] = basis[step, pl.ds(row, 16), :] * scal[pl.ds(3, 1), :]
                    return 0
                lax.fori_loop(0, BOND // 16, rescale, 0, unroll=4)

            @pl.when(blk > 0)
            def _():
                reduce(blk - 1)
            return 0

        lax.fori_loop(0, NBLK, block, 0)
        reduce(jnp.int32(NBLK - 1))

        def first(i, acc):
            row = pl.multiple_of(own0 + i * 8, 8)
            x = u[pl.ds(row, 8), :]
            return tuple(acc[m] + x * basis[m, pl.ds(row, 8), :] for m in range(KRYLOV_STEPS))
        acc = lax.fori_loop(0, ROWS // 8, first, (jnp.zeros((8, BOND), F32),) * KRYLOV_STEPS, unroll=4)
        for m in range(KRYLOV_STEPS):
            put_row(K_FIRST, m, acc[m])
        sum_start(K_FIRST)
        coef[0] = sum_finish(K_FIRST)
        mine = lax.broadcasted_iota(jnp.int32, (8, 128), 0) == step
        out_small[pl.ds(step, 1), :] = jnp.sum(jnp.where(mine, coef[0, :, 0:128], 0.0), axis=0, keepdims=True)

        def project(base, with_dots):
            def body(i, acc):
                row = pl.multiple_of(base + i * 8, 8)
                new = []
                for n in range(2):
                    cols = pl.ds(n * 384, 384)
                    x = u[pl.ds(row, 8), cols]
                    vecs = [basis[m, pl.ds(row, 8), cols] for m in range(KRYLOV_STEPS)]
                    for m in range(KRYLOV_STEPS):
                        x = x - coef[0, pl.ds(m, 1), cols] * vecs[m]
                    u[pl.ds(row, 8), cols] = x
                    if with_dots:
                        prods = [x * vec for vec in vecs] + [x * x]
                        new.append(prods)
                if not with_dots:
                    return 0
                return tuple(a + (p0 + p1) for a, p0, p1 in zip(acc, new[0], new[1]))
            init = (jnp.zeros((8, 384), F32),) * (KRYLOV_STEPS + 1) if with_dots else 0
            return lax.fori_loop(0, ROWS // 8, body, init, unroll=4)
        lax.fori_loop(0, NBLK, partner_wait, 0)
        acc = project(own0, True)
        for m in range(KRYLOV_STEPS + 1):
            put_row(K_SECOND, m, acc[m])
        sum_start(K_SECOND)
        project(oth0, False)
        total = sum_finish(K_SECOND)
        coef[1, 0:5] = total[0:5]
        scal[pl.ds(2, 1), :] = total[5:6, :]
        norm_scale()
        finalize(lax.rem(step + 1, KRYLOV_STEPS))
        return 0

    lax.fori_loop(0, KRYLOV_STEPS, krylov_step, 0)

    finish_norm(KRYLOV_STEPS)
    for copy in l_copies(0):
        copy.wait()

    def scale_out(i, _):
        row = pl.multiple_of(own0 + i * 16, 16)
        u[pl.ds(row, 16), :] = basis[0, pl.ds(row, 16), :] * scal[pl.ds(3, 1), :] * math.sqrt(4.0 * BOND * BOND)
        return 0
    lax.fori_loop(0, ROWS // 16, scale_out, 0)
    psi_out = pltpu.make_async_copy(u.at[pl.ds(own0, ROWS), :], out_psi, io_sem)
    psi_out.start()
    psi_out.wait()


def split3_xla(x):
    hi = lax.reduce_precision(x, 8, 7)
    rest = x - hi
    mid = lax.reduce_precision(rest, 8, 7)
    low = rest - mid
    return hi.astype(BF16), mid.astype(BF16), low.astype(BF16)


def mpo_matrix(w_mat):
    w0, w1, w2 = split3_xla(w_mat)
    zero = jnp.zeros_like(w0)
    return jnp.concatenate([jnp.concatenate([w0, w0, w0], axis=1),
                            jnp.concatenate([w1, w1, zero], axis=1),
                            jnp.concatenate([w2, zero, zero], axis=1)], axis=0)


def solution(mesh):
    psi_spec = P("left", None, None, "right")

    def local_fn(psi, env_left, env_right, mpo):
        odd = lax.rem(lax.axis_index("right"), 2) == 1
        psi4 = psi.reshape(ROWS, 4, COLS)
        main = jnp.where(odd, psi4[:, :, 64:], psi4[:, :, :128]).reshape(ROWS, 512)
        extra = jnp.where(odd, psi4[:, :, :64], psi4[:, :, 128:]).reshape(ROWS, 256)
        psi_q = jnp.concatenate([main, extra], axis=1)
        lefts = split3_xla(jnp.transpose(env_left, (1, 0, 2)))
        rights = split3_xla(jnp.transpose(env_right, (1, 0, 2)))
        w_rows = jnp.transpose(mpo.reshape(MPO, MPO, 4, 4), (1, 3, 2, 0)).reshape(80, 80)
        w_pairs = jnp.transpose(mpo.reshape(MPO, MPO, 2, 2, 4), (1, 4, 2, 0, 3)).reshape(80, 80)

        vmem = pl.BlockSpec(memory_space=pltpu.VMEM)
        hbm = pl.BlockSpec(memory_space=pl.ANY)
        dma = pltpu.SemaphoreType.DMA
        small, psi_new = pl.pallas_call(
            kernel,
            out_shape=(jax.ShapeDtypeStruct((16, 128), F32), jax.ShapeDtypeStruct((ROWS, BOND), F32)),
            in_specs=[hbm] * 7 + [vmem] * 2,
            out_specs=(vmem, hbm),
            scratch_shapes=[
                pltpu.VMEM((3, MPO, LB, BOND), BF16),
                pltpu.VMEM((3, MPO, 128, BOND), BF16),
                pltpu.VMEM((3, MPO, 64, BOND), BF16),
                pltpu.VMEM((3, BOND, BOND), BF16),
                pltpu.VMEM((80 * CS, 128), F32),
                pltpu.VMEM((80 * CX, 128), F32),
                pltpu.VMEM((80 * CS, 128), F32),
                pltpu.VMEM((80 * CX, 128), F32),
                pltpu.VMEM((3, 4 * LB, MPO * COLS), BF16),
                pltpu.VMEM((4 * LB, BOND), F32),
                pltpu.VMEM((2, N_RIGHT, LB, BOND), F32),
                pltpu.VMEM((N_RIGHT - 1, ROWS, BOND), F32),
                pltpu.VMEM((KRYLOV_STEPS, BOND, BOND), F32),
                pltpu.VMEM((BOND, BOND), F32),
                pltpu.VMEM((3, N_DEV, 8, 128), F32),
                pltpu.VMEM((2, 8, BOND), F32),
                pltpu.VMEM((8, BOND), F32),
                dma((3,)), dma((6,)), dma,
                dma((N_RIGHT - 1, 2)), dma((N_RIGHT - 1, NBLK)),
                dma((NBLK,)), dma((NBLK,)),
                dma((3, N_DEV - 1)), dma((3, N_DEV - 1)),
            ],
            compiler_params=pltpu.CompilerParams(
                collective_id=0, has_side_effects=True, vmem_limit_bytes=67_000_000),
            name="lanczos",
        )(psi_q, *lefts, *rights, mpo_matrix(w_rows), mpo_matrix(w_pairs))

        main = psi_new[:, :512].reshape(ROWS, 4, 128)
        extra = psi_new[:, 512:].reshape(ROWS, 4, 64)
        psi_next = jnp.where(odd, jnp.concatenate([extra, main], axis=2),
                             jnp.concatenate([main, extra], axis=2)).reshape(ROWS, 2, 2, COLS)
        return small[0:5, 0], small[9:14, 0], psi_next

    return jax.shard_map(
        local_fn,
        mesh=mesh,
        in_specs=(psi_spec, P("left", None, None), P("right", None, None), P()),
        out_specs=(P(), P(), psi_spec),
        check_vma=False,
    )
```
